32 devices in a mesh: edge: 8 (over z, y), chan: 4 (over x, core).
Axes of the slice: x: 2, y: 2, z: 4, core: 2. Of those that a mesh axis runs over, the one named last changes fastest.
Arguments:
- node_states: bfloat16 [128, 49, 256], P('edge', None, 'chan'), may hold values from -6 to 6
- edge_vectors: float32 [3, 4096], P(None, ('edge', 'chan')), may hold values from -5.6 to 5.6, as said below
- source_part: int32 [4096, 1], P('edge'), may hold values from 0 to 7; in each aligned block of 512 rows (0 to 511, 512 to 1023, ...) at most 128 rows name the same one
- source_slot: int32 [4096], P('edge'), may hold values from 0 to 15
- target_slot: int32 [4096], P('edge'), may hold values from 0 to 15
- live_edges: int32 [8], P('edge'), may hold values from 1 to 512, 3072 in all
- weight_zero: bfloat16 [7, 256, 7, 256], P(None, 'chan'), may hold values from -0.125 to 0.125
- weight_one: bfloat16 [2, 6, 256, 6, 256], P(None, None, 'chan'), may hold values from -0.109375 to 0.109375
- weight_two: bfloat16 [2, 5, 256, 5, 256], P(None, None, 'chan'), may hold values from -0.125 to 0.125
Outputs:
- aggregated: bfloat16 [128, 49, 256], P('edge', None, 'chan')
The draws below stay inside these ranges and needn't reach their ends.
Inputs may be any that keep to these rules, and one draw needn't show every extreme that they name: `source_part`: in each aligned block of 512 rows (the edges of one partition's slab) no partition number appears more than 128 times, and some number appears exactly 128 times. Edges are grouped by destination partition: the destination of an edge in slab p is node p * 16 + target_slot. `live_edges`: live slots stand at the front of each slab; the fullest slab is full. `edge_vectors`: every column has length between 0.8 and 5.6.
All inputs are finite; a program needn't handle non-finite values. No bound on the sum of `live_edges` on one device may be relied on, other than what follows from the above.
Results may differ from the reference program's by a relative error of at most 0.015.
Values may be sent and summed in bfloat16 or wider, within the bound.
A program may use at most 128 MiB of HBM per device.

```python
import math
import jax
import jax.numpy as jnp
import numpy as np
from jax import lax

C = 256
LMAX = 6
MMAX = 2
N_DEV = 16
E_CAP = 512
NODES = 128
EDGES = 4096
CAP = 128
COEFS = 49
KEPT = 29
N_EDGE = 8
N_CHAN = 4


def draw_edge_vectors(key, part):
    first_key, second_key = jax.random.split(jax.random.fold_in(key, 17))
    raw = jax.random.normal(first_key, (3, EDGES), jnp.float32)
    length = jax.random.uniform(second_key, (1, EDGES), jnp.float32, 0.8, 5.6)
    norm_value = jnp.sqrt(jnp.sum(raw * raw, axis=0, keepdims=True))
    direction = raw / jnp.maximum(norm_value, 1e-06)
    return jnp.clip(direction * length, -5.6, 5.6)


def with_ends(entries, rng, smallest, largest):
    index_at = [jax.random.randint(jax.random.fold_in(rng, axis), (), 0, length) for axis, length in enumerate(entries.shape)]
    longest = entries.shape.index(max(entries.shape))
    beside = index_at[:longest] + [(index_at[longest] + 1) % entries.shape[longest]] + index_at[longest + 1:]
    return entries.at[tuple(index_at)].set(smallest).at[tuple(beside)].set(largest)


def level_of(stream_key, shape, cuts, smallest, high):
    gain = 1.0
    for dim, shards_of in cuts:
        draws = jax.random.uniform(jax.random.fold_in(jax.random.fold_in(stream_key, 6), dim), (shards_of,), jnp.float32, smallest / len(cuts), high / len(cuts))
        gain = gain * jnp.repeat(jnp.exp(draws), shape[dim] // shards_of).reshape((-1,) + (1,) * (len(shape) - 1 - dim))
    return gain


def length_profile(number_of, total, bound, skew):
    portions = [(1 << 20) // math.isqrt(rank ** skew) + 1 for rank in range(2, number_of + 1)]
    spare, given = total - bound - (number_of - 1), [1] * (number_of - 1)
    while spare > 0:
        movable = [i for i in range(number_of - 1) if given[i] < bound]
        mass, budget = sum([portions[i] for i in movable]), spare
        for i in movable:
            more = min(bound - given[i], max(1, budget * portions[i] // mass), spare)
            given[i] = given[i] + more
            spare = spare - more
    return np.array([bound] + given)


def uneven_parts(stream_key, count, total, limit, lean):
    if count == 2:
        one = jax.random.randint(stream_key, (), max(1, total - limit), min(limit, total - 1) + 1)
        return jnp.stack([one, total - one])
    lengths = jnp.asarray(length_profile(count, total, limit, lean), jnp.int32)
    twos = (count - 1) // 2
    source_of, receiver = lengths[1:1 + 2 * twos:2], lengths[2:2 + 2 * twos:2]
    slack = jnp.minimum(source_of - 1, limit - receiver)
    passed = jax.random.randint(jax.random.fold_in(stream_key, 1), (twos,), 0, 1 << 20) % (slack + 1)
    lengths = lengths.at[1:1 + 2 * twos:2].set(source_of - passed).at[2:2 + 2 * twos:2].set(receiver + passed)
    return lengths[jax.random.permutation(jax.random.fold_in(stream_key, 2), count)]


def assign_block(own_key, own, number, rows, amount, top, most, lean):
    sequence = jax.random.permutation(own_key, amount)
    packed, usual = load_shares(amount, rows * top, most, lean, True), load_shares(amount, rows * top, most, lean, False)
    places = jnp.arange(amount)

    def named(sizes, turn):
        used = int((sizes > 0).sum())
        fixed = max(1, used // 4)
        passed = fixed + (places - fixed + turn * (used - fixed)) % max(1, amount - fixed)
        return jnp.zeros((amount,), jnp.int32).at[sequence[jnp.where(places < fixed, places, passed)]].set(jnp.asarray(sizes, jnp.int32))

    sizes = jnp.where(number % 4 == 0, named(packed, number // 4), named(usual, number - number // 4 - 1))
    mixed = jax.random.permutation(jax.random.fold_in(own, 3), amount)
    giver, receiver = mixed[0:amount // 2 * 2:2], mixed[1:amount // 2 * 2:2]
    room = jnp.minimum(sizes[giver] - 1, most - sizes[receiver]) // 2
    room = jnp.where((giver == sequence[0]) | (receiver == sequence[0]) | (sizes[receiver] == 0), 0, jnp.maximum(room, 0))
    passed = jax.random.randint(jax.random.fold_in(own, 4), (amount // 2,), 0, 1 << 20) % (room + 1)
    sizes = sizes.at[giver].add(-passed).at[receiver].add(passed)
    labels = jnp.searchsorted(jnp.cumsum(sizes), jnp.arange(rows * top), side="right").astype(jnp.int32)
    table = labels.reshape(top, rows).T
    table = table[jax.random.permutation(jax.random.fold_in(own, 1), rows)]
    turn = jax.random.randint(jax.random.fold_in(own, 2), (rows, 1), 0, top)
    return jnp.take_along_axis(table, (jnp.arange(top)[None, :] + turn) % top, axis=1)


def load_shares(count, total, bound, lean, full):
    loads = [(1 << 20) // math.isqrt(grade ** lean) + 1 for grade in range(1, count + 1)]
    largest = bound if full else min(bound, max(-(-total // count), total * loads[0] // sum(loads)))
    least = 1 if total - largest >= count - 1 else 0
    counts, rest = [largest] + [least] * (count - 1), total - largest - least * (count - 1)
    while rest > 0:
        movable = [i for i in range(1, count) if counts[i] < largest] or [i for i in range(1, count) if counts[i] < bound]
        mass, budget = sum([loads[i] for i in movable]), rest
        for i in movable:
            addition = min(bound - counts[i], max(1, budget * loads[i] // mass), rest)
            counts[i] = counts[i] + addition
            rest = rest - addition
    return np.array(counts)


def scatter_about(stream_key, shape, width, bound, cuts=(), kind=jnp.bfloat16):
    result = width * jax.random.normal(stream_key, shape, jnp.float32)
    if cuts:
        result = result * level_of(stream_key, shape, cuts, -0.22, 0.18)
    return jnp.clip(result, -bound, bound).astype(kind)


def setup_inputs(seed: int = 0) -> dict:
    splits = jax.random.split(jax.random.key(seed), 10)
    node_states = scatter_about(splits[0], (NODES, COEFS, C), 1.0, 6.0, ((0, 8), (2, 4)))
    edge_vectors = draw_edge_vectors(jax.random.fold_in(splits[9], 71), 0)
    source_part_keys = jax.random.split(jax.random.fold_in(splits[2], 1), EDGES // E_CAP)
    source_part_turns = jax.random.permutation(jax.random.fold_in(splits[2], 3), EDGES // E_CAP)
    source_part = jax.vmap(lambda own, number: assign_block(jax.random.fold_in(splits[2], 2), own, number, E_CAP, N_EDGE, 1, CAP, 2))(source_part_keys, source_part_turns).reshape((EDGES, 1))
    source_slot = with_ends(jax.random.randint(splits[3], (EDGES,), 0, N_DEV), jax.random.fold_in(splits[3], 1), 0, N_DEV - 1).astype(jnp.int32)
    target_slot = with_ends(jax.random.randint(splits[4], (EDGES,), 0, N_DEV), jax.random.fold_in(splits[4], 1), 0, N_DEV - 1).astype(jnp.int32)
    live_edges = uneven_parts(splits[5], N_EDGE, (3 * E_CAP * N_EDGE) // 4, E_CAP, 2).astype(jnp.int32)
    weight_zero = scatter_about(splits[6], (LMAX + 1, C, LMAX + 1, C), ((LMAX + 1) * C) ** -0.5, 0.125, ((1, 4),))
    weight_one = scatter_about(splits[7], (2, LMAX, C, LMAX, C), (2 * LMAX * C) ** -0.5, 0.109375, ((2, 4),))
    weight_two = scatter_about(splits[8], (2, LMAX - 1, C, LMAX - 1, C), (2 * (LMAX - 1) * C) ** -0.5, 0.125, ((2, 4),))
    return {"node_states": node_states, "edge_vectors": edge_vectors, "source_part": source_part, "source_slot": source_slot, "target_slot": target_slot, "live_edges": live_edges, "weight_zero": weight_zero, "weight_one": weight_one, "weight_two": weight_two}


cutoff_radius = 6.0
highest = lax.Precision.HIGHEST

def harmonics(coord_x, coord_y, coord_z, degree_top, order_top):
    results = {}
    real_part = [coord_x * 0.0 + 1.0]
    imag_part = [coord_x * 0.0]
    for azimuthal in range(1, order_top + 1):
        new_real = coord_x * real_part[-1] - coord_y * imag_part[-1]
        new_imag = coord_x * imag_part[-1] + coord_y * real_part[-1]
        real_part.append(new_real)
        imag_part.append(new_imag)
    for azimuthal in range(order_top + 1):
        start_value = (-1.0) ** azimuthal * math.prod(range(2 * azimuthal - 1, 0, -2))
        legendre = {azimuthal: coord_z * 0.0 + start_value}
        if azimuthal + 1 <= degree_top:
            legendre[azimuthal + 1] = coord_z * ((2 * azimuthal + 1) * start_value)
        for degree in range(azimuthal + 2, degree_top + 1):
            legendre[degree] = ((2 * degree - 1) * coord_z * legendre[degree - 1] - (degree + azimuthal - 1) * legendre[degree - 2]) / (degree - azimuthal)
        for degree in range(azimuthal, degree_top + 1):
            factor = math.sqrt((2 * degree + 1) / (4.0 * math.pi) * math.factorial(degree - azimuthal) / math.factorial(degree + azimuthal))
            if azimuthal == 0:
                results[degree, 0] = factor * legendre[degree]
            else:
                results[degree, azimuthal] = math.sqrt(2.0) * factor * legendre[degree] * real_part[azimuthal]
                results[degree, -azimuthal] = math.sqrt(2.0) * factor * legendre[degree] * imag_part[azimuthal]
    return results

def kept_rows():
    row_list = [(degree, 0) for degree in range(LMAX + 1)]
    for azimuthal in range(1, MMAX + 1):
        row_list += [(degree, azimuthal) for degree in range(azimuthal, LMAX + 1)]
        row_list += [(degree, -azimuthal) for degree in range(azimuthal, LMAX + 1)]
    return row_list

def invert_small(matrix):
    order_size = matrix.shape[0]
    work = np.concatenate([matrix, np.eye(order_size)], axis=1)
    for column in range(order_size):
        work[column] = work[column] / work[column, column]
        for row_index in range(order_size):
            if row_index != column:
                work[row_index] = work[row_index] - work[row_index, column] * work[column]
    return work[:, order_size:]

def sample_tables():
    sample_count = 2 * (LMAX + 1) ** 2
    positions = np.arange(sample_count) + 0.5
    height = 1.0 - 2.0 * positions / sample_count
    radius = np.sqrt(1.0 - height * height)
    azimuth = math.pi * (3.0 - math.sqrt(5.0)) * positions
    points = np.stack([radius * np.cos(azimuth), radius * np.sin(azimuth), height])
    values = harmonics(points[0], points[1], points[2], LMAX, LMAX)
    inverses = []
    for degree in range(LMAX + 1):
        sampled = np.stack([values[degree, azimuthal] for azimuthal in range(-degree, degree + 1)])
        inverses.append(sampled.T @ invert_small(sampled @ sampled.T))
    return (points, inverses)

def wigner_rows(vectors):
    length = jnp.sqrt(lax.optimization_barrier(jnp.sum(vectors * vectors, axis=0)))
    direction = vectors / length
    pick_first = jnp.where(jnp.abs(direction[0]) < 0.6, 1.0, 0.0).astype(jnp.float32)
    helper = jnp.stack([pick_first, 1.0 - pick_first, jnp.zeros_like(pick_first)])
    first_axis = jnp.cross(direction, helper, axis=0)
    first_axis = first_axis / jnp.sqrt(lax.optimization_barrier(jnp.sum(first_axis * first_axis, axis=0)))
    second_axis = jnp.cross(direction, first_axis, axis=0)
    frames = jnp.stack([first_axis, second_axis, direction])
    points, inverses = sample_tables()
    sample = jnp.asarray(points, jnp.float32)
    turned = jnp.einsum('rce,ck->rek', frames, sample, precision=highest)
    values = harmonics(turned[0], turned[1], turned[2], LMAX, MMAX)
    pieces = []
    for degree, azimuthal in kept_rows():
        table = jnp.asarray(inverses[degree], jnp.float32)
        pieces.append(jnp.dot(values[degree, azimuthal], table, precision=highest))
    compact = jnp.concatenate(pieces, axis=1)
    envelope = 0.5 * (jnp.cos(math.pi * length / cutoff_radius) + 1.0)
    return (compact, envelope)

def expand_rows(compact):
    padded_rows = []
    offset = 0
    for degree, azimuthal in kept_rows():
        span_size = 2 * degree + 1
        segment = compact[:, offset:offset + span_size]
        padded_rows.append(jnp.pad(segment, ((0, 0), (degree * degree, (LMAX + 1) ** 2 - degree * degree - span_size))))
        offset += span_size
    return jnp.stack(padded_rows, axis=1)

def convolve(turned, weight_zero, weight_one, weight_two, contract):
    end_zero = LMAX + 1
    end_one_plus = end_zero + LMAX
    end_one_minus = end_one_plus + LMAX
    end_two_plus = end_one_minus + LMAX - 1
    zero_part = turned[:end_zero]
    one_plus = turned[end_zero:end_one_plus]
    one_minus = turned[end_one_plus:end_one_minus]
    two_plus = turned[end_one_minus:end_two_plus]
    two_minus = turned[end_two_plus:]
    pattern = 'lce,lcjd->dje'
    out_zero = contract(pattern, zero_part, weight_zero)
    out_one_plus = contract(pattern, one_plus, weight_one[0]) - contract(pattern, one_minus, weight_one[1])
    out_one_minus = contract(pattern, one_minus, weight_one[0]) + contract(pattern, one_plus, weight_one[1])
    out_two_plus = contract(pattern, two_plus, weight_two[0]) - contract(pattern, two_minus, weight_two[1])
    out_two_minus = contract(pattern, two_minus, weight_two[0]) + contract(pattern, two_plus, weight_two[1])
    return jnp.concatenate([out_zero, out_one_plus, out_one_minus, out_two_plus, out_two_minus], axis=1)

def rounded(values):
    return lax.optimization_barrier(values.astype(jnp.bfloat16))

def float_contract(pattern, first_operand, second_operand):
    return jnp.einsum(pattern, first_operand.astype(jnp.float32), second_operand.astype(jnp.float32))

def reference(node_states, edge_vectors, source_part, source_slot, target_slot, live_edges, weight_zero, weight_one, weight_two):
    per_group = C // N_CHAN

    def one_slab(partition):
        first_edge = (partition * E_CAP).astype(jnp.int32)
        vectors = lax.dynamic_slice_in_dim(edge_vectors, first_edge, E_CAP, 1)
        compact, envelope = wigner_rows(vectors)
        rotation = expand_rows(rounded(compact))
        owner_part = lax.dynamic_slice_in_dim(source_part[:, 0], first_edge, E_CAP, 0)
        source_slots = lax.dynamic_slice_in_dim(source_slot, first_edge, E_CAP, 0)
        targets = lax.dynamic_slice_in_dim(target_slot, first_edge, E_CAP, 0)
        sources = node_states[owner_part * N_DEV + source_slots]
        turned = rounded(jnp.einsum('eik,ekc->ice', rotation.astype(jnp.float32), sources.astype(jnp.float32)))
        channel_mix = jnp.zeros((C, KEPT, E_CAP), jnp.float32)
        for group_index in range(N_CHAN):
            low_channel = group_index * per_group
            high_channel = low_channel + per_group
            partial_value = convolve(turned[:, low_channel:high_channel], weight_zero[:, low_channel:high_channel], weight_one[:, :, low_channel:high_channel], weight_two[:, :, low_channel:high_channel], float_contract)
            channel_mix = channel_mix + rounded(partial_value).astype(jnp.float32)
        alive_mask = (jnp.arange(E_CAP, dtype=jnp.int32) < live_edges[partition]).astype(jnp.float32)
        scaling = rounded(envelope).astype(jnp.float32) * alive_mask
        scaled = rounded(channel_mix * scaling)
        message = rounded(jnp.einsum('eik,cie->ekc', rotation.astype(jnp.float32), scaled.astype(jnp.float32)))
        selector = (jnp.arange(N_DEV, dtype=jnp.int32)[:, None] == targets[None, :]).astype(jnp.bfloat16)
        summed = jnp.dot(selector, message.reshape(E_CAP, COEFS * C), preferred_element_type=jnp.float32)
        return summed.astype(jnp.bfloat16).reshape(N_DEV, COEFS, C)
    blocks = lax.map(one_slab, jnp.arange(N_EDGE, dtype=jnp.int32))
    return blocks.reshape(NODES, COEFS, C)
```

```python
import math

import jax
import jax.numpy as jnp
import numpy as np
from jax import lax
from jax.experimental import pallas as pl
from jax.experimental.pallas import tpu as pltpu
from jax.sharding import PartitionSpec as P

LMAX = 6
MMAX = 2
COEFS = (LMAX + 1) ** 2
ORDERS = (0, 1, -1, 2, -2)
CUTOFF = 6.0
MESH = pl.DeviceIdType.MESH
LANES = 128


def normalizer(degree, order):
    return math.sqrt(
        (2 * degree + 1)
        / (4.0 * math.pi)
        * math.factorial(degree - order)
        / math.factorial(degree + order)
    )


def harmonics(x, y, z):
    results = {}
    power = [x * 0 + 1 + 0j]
    for _ in range(LMAX):
        power.append(power[-1] * (x + 1j * y))
    for order in range(LMAX + 1):
        start = (-1.0) ** order * math.prod(range(2 * order - 1, 0, -2))
        legendre = {order: z * 0 + start}
        if order < LMAX:
            legendre[order + 1] = (2 * order + 1) * z * start
        for degree in range(order + 2, LMAX + 1):
            legendre[degree] = (
                (2 * degree - 1) * z * legendre[degree - 1]
                - (degree + order - 1) * legendre[degree - 2]
            ) / (degree - order)
        for degree in range(order, LMAX + 1):
            value = normalizer(degree, order) * legendre[degree]
            if order == 0:
                results[degree, 0] = value
            else:
                results[degree, order] = math.sqrt(2.0) * value * power[order].real
                results[degree, -order] = math.sqrt(2.0) * value * power[order].imag
    return results


def product_tables():
    count = 4 * COEFS
    position = np.arange(count) + 0.5
    height = 1.0 - 2.0 * position / count
    radius = np.sqrt(1.0 - height * height)
    angle = math.pi * (3.0 - math.sqrt(5.0)) * position
    points = (radius * np.cos(angle), radius * np.sin(angle), height)
    values = harmonics(*points)
    names = [(degree, m) for degree in range(LMAX + 1) for m in range(-degree, degree + 1)]
    design = np.stack([values[name] for name in names], axis=1)
    inverse = np.linalg.inv(design.T @ design) @ design.T

    def expand(samples, degree):
        fitted = inverse @ samples
        span = {m: fitted[names.index((degree, m))] for m in range(-degree, degree + 1)}
        return {m: float(v) for m, v in span.items() if abs(v) > 1e-9}

    steps = {}
    for degree in range(1, LMAX + 1):
        for m in range(-(degree - 1), degree):
            for axis in range(3):
                steps[degree, m, axis] = expand(points[axis] * values[degree - 1, m], degree)
    squares = {
        (first, second): expand(points[first] * points[second], 2)
        for first in range(3)
        for second in range(3)
    }
    linear = {axis: expand(points[axis], 1) for axis in range(3)}
    return steps, squares, linear


def row_table():
    offsets, total = {}, 0
    for order in ORDERS:
        for degree in range(abs(order), LMAX + 1):
            offsets[degree, order] = total
            total += 2 * degree + 1
    return offsets, total


OFFSETS, ENTRIES = row_table()
STEPS, SQUARES, LINEAR = product_tables()


def add_terms(terms):
    total = None
    for coefficient, value in terms:
        piece = value if coefficient == 1.0 else value * coefficient
        total = piece if total is None else total + piece
    return total


def write_rotation(vx, vy, vz, rotation):
    length = jnp.sqrt(vx * vx + vy * vy + vz * vz)
    inverse = 1.0 / length
    u = (vx * inverse, vy * inverse, vz * inverse)
    first = jnp.abs(u[0]) < 0.6
    zero = jnp.zeros_like(vx)
    a = (
        jnp.where(first, zero, -u[2]),
        jnp.where(first, u[2], zero),
        jnp.where(first, -u[1], u[0]),
    )
    scale = 1.0 / jnp.sqrt(a[0] * a[0] + a[1] * a[1] + a[2] * a[2])
    a = tuple(part * scale for part in a)
    b = (
        u[1] * a[2] - u[2] * a[1],
        u[2] * a[0] - u[0] * a[2],
        u[0] * a[1] - u[1] * a[0],
    )
    axes = {1: a, -1: b}
    for order in ORDERS:
        low = abs(order)
        if order == 0:
            row = {0: jnp.ones_like(vx)}
        elif low == 1:
            unit = -math.sqrt(2.0) * normalizer(1, 1)
            row = {}
            for m in range(-1, 2):
                row[m] = add_terms(
                    [
                        (unit * LINEAR[axis][m], axes[order][axis])
                        for axis in range(3)
                        if m in LINEAR[axis]
                    ]
                )
        else:
            unit = 3.0 * math.sqrt(2.0) * normalizer(2, 2)
            pair = {}
            for i in range(3):
                for j in range(i, 3):
                    if order == 2:
                        pair[i, j] = a[i] * a[j] - b[i] * b[j]
                        weight = 1.0 if i == j else 2.0
                    else:
                        pair[i, j] = a[i] * b[j] if i == j else a[i] * b[j] + a[j] * b[i]
                        weight = 2.0
                    pair[i, j] = (weight * unit, pair[i, j])
            row = {}
            for m in range(-2, 3):
                row[m] = add_terms(
                    [
                        (factor * SQUARES[place][m], value)
                        for place, (factor, value) in pair.items()
                        if m in SQUARES[place]
                    ]
                )
        for degree in range(low, LMAX + 1):
            if degree > low:
                gain = (
                    (2 * degree - 1)
                    / (degree - low)
                    * normalizer(degree, low)
                    / normalizer(degree - 1, low)
                )
                new = {}
                for m in range(-degree, degree + 1):
                    pieces = []
                    for axis in range(3):
                        inner = [
                            (gain * STEPS[degree, source, axis][m], row[source])
                            for source in row
                            if m in STEPS[degree, source, axis]
                        ]
                        if inner:
                            pieces.append(u[axis] * add_terms(inner))
                    new[m] = sum(pieces[1:], pieces[0])
                row = new
            for m in range(-degree, degree + 1):
                rotation[OFFSETS[degree, order] + degree + m] = row[m]
    return length


def kept(degree):
    return [order for order in ORDERS if abs(order) <= degree]


GROUPS = ((0, 1, 2, 3), (4, 5), (6,))
PAIRS = (COEFS + 1) // 2


def group_span(group):
    low = group[0] ** 2
    high = (group[-1] + 1) ** 2
    return low // 2, (high + 1) // 2


def first_row(order):
    return sum(LMAX + 1 - abs(o) for o in ORDERS[: ORDERS.index(order)])


def kernel(
    sizes,
    states,
    vectors,
    part,
    slot,
    target,
    live,
    weight_zero,
    weight_one,
    weight_two,
    out,
    w0,
    w1,
    w2,
    gathered,
    spread,
    rotation,
    sources,
    turned,
    mixer0,
    mixer1,
    mixer2,
    back,
    mixed,
    outgoing,
    incoming,
    weight_sems,
    vec_send,
    vec_recv,
    line_send,
    line_recv,
    side_send,
    side_recv,
    sum_send,
    sum_recv,
):
    parts, groups, nodes, channels, slab = sizes
    mine = lax.axis_index("edge")
    chan = lax.axis_index("chan")
    side = 2 if parts % 2 == 0 else 1
    line = parts // side
    place, flank = mine // side, mine % side
    tiles = slab // LANES
    bf16, f32 = jnp.bfloat16, jnp.float32

    weight_copies = [
        pltpu.make_async_copy(source, dest, weight_sems.at[i])
        for i, (source, dest) in enumerate(
            ((weight_zero, w0), (weight_one, w1), (weight_two, w2))
        )
    ]
    for copy in weight_copies:
        copy.start()

    for pair in range(PAIRS):
        left = states[2 * pair]
        if 2 * pair + 1 < COEFS:
            right = states[2 * pair + 1]
        else:
            right = jnp.zeros_like(left)
        gathered[mine, pair] = jnp.concatenate([left, right], axis=1)
    spread[chan] = vectors[...]

    def line_at(step):
        return ((place + step) % line) * side + flank

    across = place * side + (side - 1 - flank)
    barrier = pltpu.get_barrier_semaphore()
    met = 0
    for step in range(1, line):
        pl.semaphore_signal(barrier, 1, device_id=(line_at(step), chan), device_id_type=MESH)
        met += 1
    if side == 2:
        pl.semaphore_signal(barrier, 1, device_id=(across, chan), device_id_type=MESH)
        met += 1
    for step in range(1, groups):
        pl.semaphore_signal(
            barrier, 1, device_id=(mine, (chan + step) % groups), device_id_type=MESH
        )
        met += 1
    pl.semaphore_wait(barrier, met)

    vector_copies = []
    for step in range(1, groups):
        copy = pltpu.make_async_remote_copy(
            src_ref=vectors,
            dst_ref=spread.at[chan],
            send_sem=vec_send.at[step - 1],
            recv_sem=vec_recv.at[step - 1],
            device_id=(mine, (chan + step) % groups),
            device_id_type=MESH,
        )
        copy.start()
        vector_copies.append(copy)

    line_copies, side_copies = {}, {}
    for index, group in enumerate(GROUPS):
        low, high = group_span(group)
        span = pl.ds(low, high - low)
        for step in range(line):
            if step:
                line_copies[index, step] = pltpu.make_async_remote_copy(
                    src_ref=gathered.at[mine, span],
                    dst_ref=gathered.at[mine, span],
                    send_sem=line_send.at[index, step - 1],
                    recv_sem=line_recv.at[index, step - 1],
                    device_id=(line_at(step), chan),
                    device_id_type=MESH,
                )
            if side == 2:
                owner = line_at(line - step if step else 0)
                side_copies[index, step] = pltpu.make_async_remote_copy(
                    src_ref=gathered.at[owner, span],
                    dst_ref=gathered.at[owner, span],
                    send_sem=side_send.at[index, step],
                    recv_sem=side_recv.at[index, step],
                    device_id=(across, chan),
                    device_id_type=MESH,
                )
    for index in range(len(GROUPS)):
        for step in range(line - 1, 0, -1):
            line_copies[index, step].start()
        if side == 2:
            side_copies[index, 0].start()

    def forward(index):
        for step in range(1, line):
            line_copies[index, step].wait_recv()
            if side == 2:
                side_copies[index, step].start()

    for copy in vector_copies:
        copy.wait_recv()
    length = write_rotation(spread[:, 0, :], spread[:, 1, :], spread[:, 2, :], rotation)
    number = (
        lax.broadcasted_iota(jnp.int32, (tiles, LANES), 0) * LANES
        + lax.broadcasted_iota(jnp.int32, (tiles, LANES), 1)
    )
    envelope = 0.5 * (jnp.cos(length * (math.pi / CUTOFF)) + 1.0)
    fade = jnp.where(number < live[0], envelope, 0.0)
    forward(0)

    row = 0
    for tile in range(tiles):
        lanes = pl.ds(tile * LANES, LANES)
        hit = lax.broadcasted_iota(jnp.int32, (nodes, LANES), 0) == target[:, lanes]
        chosen = jnp.where(hit, jnp.broadcast_to(fade[tile : tile + 1], (nodes, LANES)), 0.0)
        for degree in range(LMAX + 1):
            for place_of, order in enumerate(kept(degree)):
                columns = pl.ds(place_of * slab + tile * LANES, LANES)
                for inner in range(2 * degree + 1):
                    entry = rotation[OFFSETS[degree, order] + inner, tile : tile + 1, :]
                    rows = pl.ds((degree * degree + inner) * nodes, nodes)
                    back[rows, columns] = (chosen * entry).astype(bf16)
        if tile == 0:
            forward(1)
        if tile == min(1, tiles - 1):
            forward(2)

    everyone = parts * nodes
    wanted = part[...] * nodes + slot[...]
    picker = jnp.where(
        lax.broadcasted_iota(jnp.int32, (everyone, slab), 0) == wanted, 1.0, 0.0
    ).astype(bf16)

    half = 16
    for index, group in enumerate(GROUPS):
        if side == 2:
            for step in range(line):
                side_copies[index, step].wait_recv()
        low, high = group_span(group)
        for pair in range(low, high):
            table = gathered[:, pair].reshape(everyone, 2 * channels)
            picked = lax.dot_general(
                table, picker, (((0,), (0,)), ((), ())), preferred_element_type=f32
            )
            sources[pl.ds(pair * 2 * channels, 2 * channels), :] = picked

        def turn(step, carry, group=group):
            start = pl.multiple_of((step // tiles) * half, half)
            tile = step % tiles
            lanes = pl.ds(pl.multiple_of(tile * LANES, LANES), LANES)
            for degree in group:
                totals = {}
                for inner in range(2 * degree + 1):
                    coefficient = degree * degree + inner
                    value = sources[pl.ds(coefficient * channels + start, half), lanes]
                    for order in kept(degree):
                        entry = rotation[OFFSETS[degree, order] + inner, pl.ds(tile, 1), :]
                        term = entry * value
                        totals[order] = term if inner == 0 else totals[order] + term
                for order in kept(degree):
                    at = (first_row(order) + degree - abs(order)) * channels
                    turned[pl.ds(at + start, half), lanes] = totals[order].astype(bf16)
            return carry

        lax.fori_loop(0, tiles * (channels // half), turn, 0)

    def eye(sign):
        same = lax.broadcasted_iota(jnp.int32, (slab, slab), 0) == lax.broadcasted_iota(
            jnp.int32, (slab, slab), 1
        )
        return jnp.where(same, sign, 0.0).astype(bf16)

    def flip(order):
        count = (LMAX + 1 - abs(order)) * channels
        return turned[pl.ds(first_row(order) * channels, count), :].T

    mixer0[...] = flip(0)
    for mixer, order in ((mixer1, 1), (mixer2, 2)):
        width = (LMAX + 1 - order) * channels
        plus, minus = flip(order), flip(-order)
        mixer[0:slab, 0:width] = plus
        mixer[0:slab, width : 2 * width] = -minus
        mixer[slab : 2 * slab, 0:width] = minus
        mixer[slab : 2 * slab, width : 2 * width] = plus

    for copy in weight_copies:
        copy.wait()

    width = groups * channels
    fold = LANES // channels
    sum_copies = {}
    low_lanes = lax.broadcasted_iota(jnp.int32, (1, LANES), 1) < channels
    for degree in range(LMAX, -1, -1):
        mixed[0:slab] = jnp.dot(
            mixer0[...], w0[:, degree].reshape(-1, width), preferred_element_type=f32
        ).astype(bf16)
        for order, mixer, weight in ((1, mixer1, w1), (2, mixer2, w2)):
            if degree >= order:
                at = (2 * order - 1) * slab
                mixed[at : at + 2 * slab] = jnp.dot(
                    mixer[...],
                    weight[:, :, degree - order].reshape(-1, width),
                    preferred_element_type=f32,
                ).astype(bf16)
        used = len(kept(degree)) * slab
        height = (2 * degree + 1) * nodes
        top = degree * degree * nodes
        total = jnp.dot(
            back[top : top + height, 0:used], mixed[0:used], preferred_element_type=f32
        )
        short = height // fold
        begin = top // fold
        for lump in range(width // LANES):
            block = total[:, lump * LANES : (lump + 1) * LANES]
            upper, lower = block[:short], block[short:]
            even = jnp.where(low_lanes, upper, pltpu.roll(lower, channels, 1))
            odd = jnp.where(low_lanes, pltpu.roll(upper, channels, 1), lower)
            outgoing[2 * lump, begin : begin + short] = even.astype(bf16)
            outgoing[2 * lump + 1, begin : begin + short] = odd.astype(bf16)
        for step in range(1, groups):
            peer = (chan + step) % groups
            copy = pltpu.make_async_remote_copy(
                src_ref=outgoing.at[peer, pl.ds(begin, short)],
                dst_ref=incoming.at[step - 1, pl.ds(begin, short)],
                send_sem=sum_send.at[degree, step - 1],
                recv_sem=sum_recv.at[degree, step - 1],
                device_id=(mine, peer),
                device_id_type=MESH,
            )
            copy.start()
            sum_copies[degree, step] = copy

    for degree in range(LMAX, -1, -1):
        height = (2 * degree + 1) * nodes
        top = degree * degree * nodes
        short = height // fold
        begin = top // fold
        total = outgoing[chan, begin : begin + short].astype(f32)
        for step in range(1, groups):
            sum_copies[degree, step].wait_recv()
            total = total + incoming[step - 1, begin : begin + short].astype(f32)
        out[top : top + short] = total[:, :channels].astype(bf16)
        out[top + short : top + height] = pltpu.roll(total, channels, 1)[:, :channels].astype(bf16)

    for copy in vector_copies:
        copy.wait_send()
    for copy in line_copies.values():
        copy.wait_send()
    for copy in side_copies.values():
        copy.wait_send()
    for copy in sum_copies.values():
        copy.wait_send()


def shards(
    node_states,
    edge_vectors,
    source_part,
    source_slot,
    target_slot,
    live_edges,
    weight_zero,
    weight_one,
    weight_two,
):
    slab = source_slot.shape[0]
    nodes, coefs, channels = node_states.shape
    parts = lax.axis_size("edge")
    groups = lax.axis_size("chan")
    side = 2 if parts % 2 == 0 else 1
    line = parts // side
    tiles = slab // LANES
    width = groups * channels
    bf16, f32 = jnp.bfloat16, jnp.float32
    sizes = (parts, groups, nodes, channels, slab)

    def body(*refs):
        kernel(sizes, *refs)

    vmem = pl.BlockSpec(memory_space=pltpu.VMEM)
    anywhere = pl.BlockSpec(memory_space=pl.ANY)
    zero = weight_zero.transpose(0, 2, 1, 3)
    one = weight_one.transpose(0, 1, 3, 2, 4)
    two = weight_two.transpose(0, 1, 3, 2, 4)
    dma = pltpu.SemaphoreType.DMA
    lots = len(GROUPS)
    result = pl.pallas_call(
        body,
        in_specs=[
            vmem,
            vmem,
            vmem,
            vmem,
            vmem,
            pl.BlockSpec(memory_space=pltpu.SMEM),
            anywhere,
            anywhere,
            anywhere,
        ],
        out_specs=vmem,
        out_shape=jax.ShapeDtypeStruct((coefs * nodes, channels), bf16),
        scratch_shapes=[
            pltpu.VMEM(zero.shape, bf16),
            pltpu.VMEM(one.shape, bf16),
            pltpu.VMEM(two.shape, bf16),
            pltpu.VMEM((parts, PAIRS, nodes, 2 * channels), bf16),
            pltpu.VMEM((groups, 3, slab // groups), f32),
            pltpu.VMEM((ENTRIES, tiles, LANES), f32),
            pltpu.VMEM((2 * PAIRS * channels, slab), f32),
            pltpu.VMEM(((first_row(-2) + LMAX - 1) * channels, slab), bf16),
            pltpu.VMEM((slab, (LMAX + 1) * channels), bf16),
            pltpu.VMEM((2 * slab, 2 * LMAX * channels), bf16),
            pltpu.VMEM((2 * slab, 2 * (LMAX - 1) * channels), bf16),
            pltpu.VMEM((coefs * nodes, len(ORDERS) * slab), bf16),
            pltpu.VMEM((len(ORDERS) * slab, width), bf16),
            pltpu.VMEM((groups, coefs * nodes * channels // LANES, LANES), bf16),
            pltpu.VMEM((groups - 1, coefs * nodes * channels // LANES, LANES), bf16),
            dma((3,)),
            dma((groups - 1,)),
            dma((groups - 1,)),
            dma((lots, max(line - 1, 1))),
            dma((lots, max(line - 1, 1))),
            dma((lots, line)),
            dma((lots, line)),
            dma((LMAX + 1, groups - 1)),
            dma((LMAX + 1, groups - 1)),
        ],
        compiler_params=pltpu.CompilerParams(
            collective_id=0, has_side_effects=True, vmem_limit_bytes=60 * 1024 * 1024
        ),
        name="message_layer",
    )(
        node_states.transpose(1, 0, 2),
        edge_vectors,
        source_part.reshape(1, slab),
        source_slot.reshape(1, slab),
        target_slot.reshape(1, slab),
        live_edges,
        zero,
        one,
        two,
    )
    return result.reshape(coefs, nodes, channels).transpose(1, 0, 2)


def solution(mesh):
    in_specs = (
        P("edge", None, "chan"),
        P(None, ("edge", "chan")),
        P("edge", None),
        P("edge"),
        P("edge"),
        P("edge"),
        P(None, "chan", None, None),
        P(None, None, "chan", None, None),
        P(None, None, "chan", None, None),
    )
    out_specs = P("edge", None, "chan")
    return jax.shard_map(shards, mesh=mesh, in_specs=in_specs, out_specs=out_specs, check_vma=False)
```

```python
import math

import jax
import jax.numpy as jnp
import numpy as np
from jax import lax
from jax.experimental import pallas as pl
from jax.experimental.pallas import tpu as pltpu
from jax.sharding import PartitionSpec as P

LMAX = 6
MMAX = 2
COEFS = (LMAX + 1) ** 2
ORDERS = (0, 1, -1, 2, -2)
CUTOFF = 6.0
MESH = pl.DeviceIdType.MESH
LANES = 128


def normalizer(degree, order):
    return math.sqrt(
        (2 * degree + 1)
        / (4.0 * math.pi)
        * math.factorial(degree - order)
        / math.factorial(degree + order)
    )


def harmonics(x, y, z):
    results = {}
    power = [x * 0 + 1 + 0j]
    for _ in range(LMAX):
        power.append(power[-1] * (x + 1j * y))
    for order in range(LMAX + 1):
        start = (-1.0) ** order * math.prod(range(2 * order - 1, 0, -2))
        legendre = {order: z * 0 + start}
        if order < LMAX:
            legendre[order + 1] = (2 * order + 1) * z * start
        for degree in range(order + 2, LMAX + 1):
            legendre[degree] = (
                (2 * degree - 1) * z * legendre[degree - 1]
                - (degree + order - 1) * legendre[degree - 2]
            ) / (degree - order)
        for degree in range(order, LMAX + 1):
            value = normalizer(degree, order) * legendre[degree]
            if order == 0:
                results[degree, 0] = value
            else:
                results[degree, order] = math.sqrt(2.0) * value * power[order].real
                results[degree, -order] = math.sqrt(2.0) * value * power[order].imag
    return results


def product_tables():
    count = 4 * COEFS
    position = np.arange(count) + 0.5
    height = 1.0 - 2.0 * position / count
    radius = np.sqrt(1.0 - height * height)
    angle = math.pi * (3.0 - math.sqrt(5.0)) * position
    points = (radius * np.cos(angle), radius * np.sin(angle), height)
    values = harmonics(*points)
    names = [(degree, m) for degree in range(LMAX + 1) for m in range(-degree, degree + 1)]
    design = np.stack([values[name] for name in names], axis=1)
    inverse = np.linalg.inv(design.T @ design) @ design.T

    def expand(samples, degree):
        fitted = inverse @ samples
        span = {m: fitted[names.index((degree, m))] for m in range(-degree, degree + 1)}
        return {m: float(v) for m, v in span.items() if abs(v) > 1e-9}

    steps = {}
    for degree in range(1, LMAX + 1):
        for m in range(-(degree - 1), degree):
            for axis in range(3):
                steps[degree, m, axis] = expand(points[axis] * values[degree - 1, m], degree)
    squares = {
        (first, second): expand(points[first] * points[second], 2)
        for first in range(3)
        for second in range(3)
    }
    linear = {axis: expand(points[axis], 1) for axis in range(3)}
    return steps, squares, linear


def row_table():
    offsets, total = {}, 0
    for order in ORDERS:
        for degree in range(abs(order), LMAX + 1):
            offsets[degree, order] = total
            total += 2 * degree + 1
    return offsets, total


OFFSETS, ENTRIES = row_table()
STEPS, SQUARES, LINEAR = product_tables()


def add_terms(terms):
    total = None
    for coefficient, value in terms:
        piece = value if coefficient == 1.0 else value * coefficient
        total = piece if total is None else total + piece
    return total


def write_rotation(vx, vy, vz, rotation, orders):
    length = jnp.sqrt(vx * vx + vy * vy + vz * vz)
    inverse = 1.0 / length
    u = (vx * inverse, vy * inverse, vz * inverse)
    first = jnp.abs(u[0]) < 0.6
    zero = jnp.zeros_like(vx)
    a = (
        jnp.where(first, zero, -u[2]),
        jnp.where(first, u[2], zero),
        jnp.where(first, -u[1], u[0]),
    )
    scale = 1.0 / jnp.sqrt(a[0] * a[0] + a[1] * a[1] + a[2] * a[2])
    a = tuple(part * scale for part in a)
    b = (
        u[1] * a[2] - u[2] * a[1],
        u[2] * a[0] - u[0] * a[2],
        u[0] * a[1] - u[1] * a[0],
    )
    axes = {1: a, -1: b}
    for order in orders:
        low = abs(order)
        if order == 0:
            row = {0: jnp.ones_like(vx)}
        elif low == 1:
            unit = -math.sqrt(2.0) * normalizer(1, 1)
            row = {}
            for m in range(-1, 2):
                row[m] = add_terms(
                    [
                        (unit * LINEAR[axis][m], axes[order][axis])
                        for axis in range(3)
                        if m in LINEAR[axis]
                    ]
                )
        else:
            unit = 3.0 * math.sqrt(2.0) * normalizer(2, 2)
            pair = {}
            for i in range(3):
                for j in range(i, 3):
                    if order == 2:
                        pair[i, j] = a[i] * a[j] - b[i] * b[j]
                        weight = 1.0 if i == j else 2.0
                    else:
                        pair[i, j] = a[i] * b[j] if i == j else a[i] * b[j] + a[j] * b[i]
                        weight = 2.0
                    pair[i, j] = (weight * unit, pair[i, j])
            row = {}
            for m in range(-2, 3):
                row[m] = add_terms(
                    [
                        (factor * SQUARES[place][m], value)
                        for place, (factor, value) in pair.items()
                        if m in SQUARES[place]
                    ]
                )
        for degree in range(low, LMAX + 1):
            if degree > low:
                gain = (
                    (2 * degree - 1)
                    / (degree - low)
                    * normalizer(degree, low)
                    / normalizer(degree - 1, low)
                )
                new = {}
                for m in range(-degree, degree + 1):
                    pieces = []
                    for axis in range(3):
                        inner = [
                            (gain * STEPS[degree, source, axis][m], row[source])
                            for source in row
                            if m in STEPS[degree, source, axis]
                        ]
                        if inner:
                            pieces.append(u[axis] * add_terms(inner))
                    new[m] = sum(pieces[1:], pieces[0])
                row = new
            for m in range(-degree, degree + 1):
                rotation[OFFSETS[degree, order] + degree + m] = row[m]
    return length


def kept(degree):
    return [order for order in ORDERS if abs(order) <= degree]


GROUPS = ((0, 1, 2, 3), (4, 5), (6,))
PAIRS = (COEFS + 1) // 2
CHUNK = 32
COPIED = 16


def group_span(group):
    low = group[0] ** 2
    high = (group[-1] + 1) ** 2
    return low // 2, (high + 1) // 2


def contracted(size):
    listing, spans = [], []
    for group in GROUPS:
        begin = len(listing)
        for sign in (1, -1) if size else (1,):
            listing += [(degree, sign) for degree in group if degree >= size]
        spans.append((begin, len(listing)))
    return listing, spans


LISTS = [contracted(size) for size in range(MMAX + 1)]


def weight_plan(size):
    plan = []
    for minus in (0, 1):
        slot = 0
        for group in GROUPS:
            used = [degree for degree in group if degree >= size]
            for part in (0, 1):
                plan.append((minus, part ^ minus, used[0] - size, len(used), slot))
                slot += len(used)
    return plan


class Refs:
    pass


def kernel(sizes, names, *refs):
    r = Refs()
    for name, ref in zip(names, refs):
        setattr(r, name, ref)
    parts, groups, nodes, channels, slab = sizes
    mine = lax.axis_index("edge")
    chan = lax.axis_index("chan")
    side = 2 if parts % 2 == 0 else 1
    line = parts // side
    place, flank = mine // side, mine % side
    tiles = slab // LANES
    bf16, f32 = jnp.bfloat16, jnp.float32
    width = groups * channels
    across = place * side + (side - 1 - flank)

    def at(where):
        return where * side + flank

    loads = [
        pltpu.make_async_copy(source, dest, r.load_sems.at[k])
        for k, (source, dest) in enumerate(
            (
                (r.states_hbm, r.states),
                (r.vectors_hbm, r.vectors),
                (r.part_hbm, r.part),
                (r.slot_hbm, r.slot),
                (r.target_hbm, r.target),
                (r.live_hbm, r.live),
            )
        )
    ]
    for copy in loads:
        copy.start()

    barrier = pltpu.get_barrier_semaphore()
    reach = min(2, line - 1)
    met = 0
    for step in range(1, reach + 1):
        for way in (-1, 1):
            there = place + way * step
            present = (there >= 0) & (there < line)

            @pl.when(present)
            def _(there=there):
                pl.semaphore_signal(barrier, 1, device_id=(at(there), chan), device_id_type=MESH)

            met = met + jnp.where(present, 1, 0)
    if side == 2:
        pl.semaphore_signal(barrier, 1, device_id=(across, chan), device_id_type=MESH)
        met = met + 1
    for step in range(1, groups):
        peer = (chan + step) % groups
        pl.semaphore_signal(barrier, 1, device_id=(mine, peer), device_id_type=MESH)
        met = met + 1

    weight_copies = [pltpu.make_async_copy(r.weight_zero, r.w0, r.weight_sems.at[0])]
    for size, source, dests in (
        (1, r.weight_one, (r.plus1, r.minus1)),
        (2, r.weight_two, (r.plus2, r.minus2)),
    ):
        for minus, part, low, count, slot in weight_plan(size):
            weight_copies.append(
                pltpu.make_async_copy(
                    source.at[part, pl.ds(low, count)],
                    dests[minus].at[pl.ds(slot, count)],
                    r.weight_sems.at[len(weight_copies)],
                )
            )
    for copy in weight_copies:
        copy.start()

    loads[0].wait()
    for pair in range(PAIRS):
        left = r.states[2 * pair]
        if 2 * pair + 1 < COEFS:
            right = r.states[2 * pair + 1]
        else:
            right = jnp.zeros_like(left)
        r.gathered[mine, pair] = jnp.concatenate([left, right], axis=1)
    for copy in loads[1:]:
        copy.wait()
    r.spread[chan] = r.vectors[...]
    pl.semaphore_wait(barrier, met)

    vector_copies = []
    for step in range(1, groups):
        copy = pltpu.make_async_remote_copy(
            src_ref=r.vectors,
            dst_ref=r.spread.at[chan],
            send_sem=r.vec_send.at[step - 1],
            recv_sem=r.vec_recv.at[step - 1],
            device_id=(mine, (chan + step) % groups),
            device_id_type=MESH,
        )
        copy.start()
        vector_copies.append(copy)

    def inside(where):
        return (where >= 0) & (where < line)

    def block_of(index, owner):
        low, high = group_span(GROUPS[index])
        return r.gathered.at[owner, pl.ds(low, high - low)]

    def along(index, way, step, jump):
        kind = (0 if way > 0 else 1, step + jump - 1)
        block = block_of(index, at(place - way * step))
        return pltpu.make_async_remote_copy(
            src_ref=block,
            dst_ref=block,
            send_sem=r.line_send.at[(index, *kind)],
            recv_sem=r.line_recv.at[(index, *kind)],
            device_id=(at(place + way * jump), chan),
            device_id_type=MESH,
        )

    def over(index, way, step):
        block = block_of(index, at(place - way * step))
        number = 0 if step == 0 else 2 * step - (1 if way > 0 else 0)
        return pltpu.make_async_remote_copy(
            src_ref=block,
            dst_ref=block,
            send_sem=r.side_send.at[index, number],
            recv_sem=r.side_recv.at[index, number],
            device_id=(across, chan),
            device_id_type=MESH,
        )

    everything = []

    def launch(present, copy):
        everything.append((present, copy))

        @pl.when(present)
        def _():
            copy.start()

    for index in range(len(GROUPS)):
        for jump in range(reach, 0, -1):
            for way in (1, -1):
                launch(inside(place + way * jump), along(index, way, 0, jump))
        if side == 2:
            over(index, 1, 0).start()

    def forward(step, index):
        for way in (1, -1):
            present = inside(place - way * step)
            onward = present & inside(place + way)

            @pl.when(present)
            def _(way=way):
                along(index, way, step - 1, 1).wait_recv()
                if side == 2:
                    over(index, way, step).start()

            if step >= 2 and step < line - 1:
                launch(onward, along(index, way, step, 1))

    def arrived(index):
        if side == 2:
            over(index, 1, 0).wait_recv()
            for step in range(1, line):
                for way in (1, -1):

                    @pl.when(inside(place - way * step))
                    def _(way=way, step=step):
                        over(index, way, step).wait_recv()

    for copy in vector_copies:
        copy.wait_recv()
    number = (
        lax.broadcasted_iota(jnp.int32, (tiles, LANES), 0) * LANES
        + lax.broadcasted_iota(jnp.int32, (tiles, LANES), 1)
    )

    def prepare(step):
        if step < len(ORDERS):
            length = write_rotation(
                r.spread[:, 0, :], r.spread[:, 1, :], r.spread[:, 2, :], r.rotation, (ORDERS[step],)
            )
            if step == 0:
                envelope = 0.5 * (jnp.cos(length * (math.pi / CUTOFF)) + 1.0)
                r.fade[...] = jnp.where(number < r.live[0], envelope, 0.0)
        elif step < len(ORDERS) + tiles:
            tile = step - len(ORDERS)
            lanes = pl.ds(tile * LANES, LANES)
            hit = lax.broadcasted_iota(jnp.int32, (nodes, LANES), 0) == r.target[:, lanes]
            fading = jnp.broadcast_to(r.fade[tile : tile + 1], (nodes, LANES))
            chosen = jnp.where(hit, fading, 0.0).astype(bf16)
            for degree in range(LMAX + 1):
                for place_of, order in enumerate(kept(degree)):
                    columns = pl.ds(place_of * slab + tile * LANES, LANES)
                    for inner in range(2 * degree + 1):
                        entry = OFFSETS[degree, order] + inner
                        row = jnp.broadcast_to(
                            r.rotation[entry, tile : tile + 1, :], (COPIED, LANES)
                        ).astype(bf16)
                        r.copied[entry, :, lanes] = row
                        rows = pl.ds((degree * degree + inner) * nodes, nodes)
                        r.back[rows, columns] = chosen * row

    steps = [(step, index) for step in range(1, line) for index in range(len(GROUPS))]
    chores = len(ORDERS) + tiles
    done = 0
    for count, (step, index) in enumerate(steps):
        forward(step, index)
        while done < chores and done <= count:
            prepare(done)
            done += 1
    while done < chores:
        prepare(done)
        done += 1

    everyone = parts * nodes
    wanted = r.part[...] * nodes + r.slot[...]
    picker = jnp.where(
        lax.broadcasted_iota(jnp.int32, (everyone, slab), 0) == wanted, 1.0, 0.0
    ).astype(bf16)

    turned = (r.turned0, r.turned1, r.turned2)
    mixers = (r.mixer0, r.mixer1, r.mixer2)
    for index, group in enumerate(GROUPS):
        arrived(index)
        low, high = group_span(group)
        for pair in range(low, high):
            table = r.gathered[:, pair].reshape(everyone, 2 * channels)
            picked = lax.dot_general(
                table, picker, (((0,), (0,)), ((), ())), preferred_element_type=f32
            )
            r.sources[pl.ds(pair * 2 * channels, 2 * channels), :] = picked.astype(bf16)

        def turn(step, carry, group=group):
            start = pl.multiple_of((step // tiles) * CHUNK, CHUNK)
            lanes = pl.ds(pl.multiple_of((step % tiles) * LANES, LANES), LANES)
            for degree in group:
                totals = {}
                for inner in range(2 * degree + 1):
                    coefficient = degree * degree + inner
                    value = r.sources[pl.ds(coefficient * channels + start, CHUNK), lanes]
                    value = value.reshape(CHUNK // COPIED, COPIED, LANES)
                    for order in kept(degree):
                        entry = r.copied[OFFSETS[degree, order] + inner, :, lanes]
                        term = entry[None] * value
                        totals[order] = term if inner == 0 else totals[order] + term
                for order in kept(degree):
                    sign = -1 if order < 0 else 1
                    row = LISTS[abs(order)][0].index((degree, sign)) * channels
                    turned[abs(order)][pl.ds(row + start, CHUNK), lanes] = totals[order].reshape(
                        CHUNK, LANES
                    )
            return carry

        lax.fori_loop(0, tiles * (channels // CHUNK), turn, 0)
        for size in range(MMAX + 1):
            begin, end = (n * channels for n in LISTS[size][1][index])
            mixers[size][:, begin:end] = turned[size][begin:end, :].T

    for copy in weight_copies:
        copy.wait()
    for size, weights in ((1, r.plus1), (2, r.plus2)):
        for slot, (_, sign) in enumerate(LISTS[size][0]):
            if sign < 0:
                weights[slot] = -weights[slot]

    fold = LANES // channels
    low_lanes = lax.broadcasted_iota(jnp.int32, (1, LANES), 1) < channels

    def span_of(degree):
        height = (2 * degree + 1) * nodes
        top = degree * degree * nodes
        return top, height, top // fold, height // fold

    def convolve(degree):
        keep = degree % 2
        for number, order in enumerate(kept(degree)):
            size = abs(order)
            if size == 0:
                weight = r.w0[:, degree]
            else:
                source = ((r.minus1, r.plus1), (r.minus2, r.plus2))[size - 1][order > 0]
                weight = source[:, degree - size]
            r.mixed[keep, number * slab : (number + 1) * slab] = jnp.dot(
                mixers[size][...], weight.reshape(-1, width), preferred_element_type=f32
            ).astype(bf16)

    def gather_back(degree):
        used = len(kept(degree)) * slab
        top, height, begin, short = span_of(degree)
        total = jnp.dot(
            r.back[top : top + height, 0:used],
            r.mixed[degree % 2, 0:used],
            preferred_element_type=f32,
        )
        for lump in range(width // LANES):
            block = total[:, lump * LANES : (lump + 1) * LANES]
            upper, lower = block[:short], block[short:]
            even = jnp.where(low_lanes, upper, pltpu.roll(lower, channels, 1))
            odd = jnp.where(low_lanes, pltpu.roll(upper, channels, 1), lower)
            r.outgoing[2 * lump, begin : begin + short] = even.astype(bf16)
            r.outgoing[2 * lump + 1, begin : begin + short] = odd.astype(bf16)

    sum_copies = {}

    def send(degree):
        _, _, begin, short = span_of(degree)
        for step in range(1, groups):
            peer = (chan + step) % groups
            copy = pltpu.make_async_remote_copy(
                src_ref=r.outgoing.at[peer, pl.ds(begin, short)],
                dst_ref=r.incoming.at[step - 1, pl.ds(begin, short)],
                send_sem=r.sum_send.at[degree, step - 1],
                recv_sem=r.sum_recv.at[degree, step - 1],
                device_id=(mine, peer),
                device_id_type=MESH,
            )
            copy.start()
            sum_copies[degree, step] = copy

    for degree in range(LMAX, -1, -1):
        if degree + 2 <= LMAX:
            send(degree + 2)
        convolve(degree)
        if degree + 1 <= LMAX:
            gather_back(degree + 1)
    send(1)
    gather_back(0)
    send(0)

    for degree in range(LMAX, -1, -1):
        top, height, begin, short = span_of(degree)
        total = r.outgoing[chan, begin : begin + short].astype(f32)
        for step in range(1, groups):
            sum_copies[degree, step].wait_recv()
            total = total + r.incoming[step - 1, begin : begin + short].astype(f32)
        r.out[top : top + short] = total[:, :channels].astype(bf16)
        r.out[top + short : top + height] = pltpu.roll(total, channels, 1)[:, :channels].astype(
            bf16
        )

    for copy in vector_copies:
        copy.wait_send()
    for present, copy in everything:

        @pl.when(present)
        def _(copy=copy):
            copy.wait_send()

    if side == 2:
        for index in range(len(GROUPS)):
            over(index, 1, 0).wait_send()
            for step in range(1, line):
                for way in (1, -1):

                    @pl.when(inside(place - way * step))
                    def _(index=index, way=way, step=step):
                        over(index, way, step).wait_send()

    for copy in sum_copies.values():
        copy.wait_send()


def shards(
    node_states,
    edge_vectors,
    source_part,
    source_slot,
    target_slot,
    live_edges,
    weight_zero,
    weight_one,
    weight_two,
):
    slab = source_slot.shape[0]
    nodes, coefs, channels = node_states.shape
    parts = lax.axis_size("edge")
    groups = lax.axis_size("chan")
    line = parts // (2 if parts % 2 == 0 else 1)
    tiles = slab // LANES
    width = groups * channels
    bf16, f32, i32 = jnp.bfloat16, jnp.float32, jnp.int32
    zero = weight_zero.transpose(0, 2, 1, 3)
    one = weight_one.transpose(0, 1, 3, 2, 4)
    two = weight_two.transpose(0, 1, 3, 2, 4)
    operands = dict(
        states_hbm=node_states.transpose(1, 0, 2),
        vectors_hbm=edge_vectors,
        part_hbm=source_part.reshape(1, slab),
        slot_hbm=source_slot.reshape(1, slab),
        target_hbm=target_slot.reshape(1, slab),
        live_hbm=live_edges,
        weight_zero=zero,
        weight_one=one,
        weight_two=two,
    )
    dma = pltpu.SemaphoreType.DMA
    vmem = pltpu.VMEM
    lots = len(GROUPS)
    rows = [len(listing) * channels for listing, _ in LISTS]
    hops = max(line - 1, 1)
    folded = coefs * nodes * channels // LANES
    weight_shape = [(len(listing),) for listing, _ in LISTS]
    scratch = dict(
        states=vmem((coefs, nodes, channels), bf16),
        vectors=vmem(edge_vectors.shape, f32),
        part=vmem((1, slab), i32),
        slot=vmem((1, slab), i32),
        target=vmem((1, slab), i32),
        live=pltpu.SMEM((1,), i32),
        w0=vmem(zero.shape, bf16),
        plus1=vmem(weight_shape[1] + one.shape[2:], bf16),
        minus1=vmem(weight_shape[1] + one.shape[2:], bf16),
        plus2=vmem(weight_shape[2] + two.shape[2:], bf16),
        minus2=vmem(weight_shape[2] + two.shape[2:], bf16),
        gathered=vmem((parts, PAIRS, nodes, 2 * channels), bf16),
        spread=vmem((groups, 3, slab // groups), f32),
        rotation=vmem((ENTRIES, tiles, LANES), f32),
        fade=vmem((tiles, LANES), f32),
        copied=vmem((ENTRIES, COPIED, slab), bf16),
        sources=vmem((2 * PAIRS * channels, slab), bf16),
        turned0=vmem((rows[0], slab), bf16),
        turned1=vmem((rows[1], slab), bf16),
        turned2=vmem((rows[2], slab), bf16),
        mixer0=vmem((slab, rows[0]), bf16),
        mixer1=vmem((slab, rows[1]), bf16),
        mixer2=vmem((slab, rows[2]), bf16),
        back=vmem((coefs * nodes, len(ORDERS) * slab), bf16),
        mixed=vmem((2, len(ORDERS) * slab, width), bf16),
        outgoing=vmem((groups, folded, LANES), bf16),
        incoming=vmem((groups - 1, folded, LANES), bf16),
        load_sems=dma((6,)),
        weight_sems=dma((1 + len(weight_plan(1)) + len(weight_plan(2)),)),
        vec_send=dma((groups - 1,)),
        vec_recv=dma((groups - 1,)),
        line_send=dma((lots, 2, hops)),
        line_recv=dma((lots, 2, hops)),
        side_send=dma((lots, 2 * line - 1)),
        side_recv=dma((lots, 2 * line - 1)),
        sum_send=dma((LMAX + 1, groups - 1)),
        sum_recv=dma((LMAX + 1, groups - 1)),
    )
    names = [*operands, "out", *scratch]
    sizes = (parts, groups, nodes, channels, slab)

    def body(*refs):
        kernel(sizes, names, *refs)

    result = pl.pallas_call(
        body,
        in_specs=[pl.BlockSpec(memory_space=pl.ANY)] * len(operands),
        out_specs=pl.BlockSpec(memory_space=pltpu.VMEM),
        out_shape=jax.ShapeDtypeStruct((coefs * nodes, channels), bf16),
        scratch_shapes=list(scratch.values()),
        compiler_params=pltpu.CompilerParams(
            collective_id=0, has_side_effects=True, vmem_limit_bytes=48 * 1024 * 1024
        ),
        name="message_layer",
    )(*operands.values())
    return result.reshape(coefs, nodes, channels).transpose(1, 0, 2)


def solution(mesh):
    in_specs = (
        P("edge", None, "chan"),
        P(None, ("edge", "chan")),
        P("edge", None),
        P("edge"),
        P("edge"),
        P("edge"),
        P(None, "chan", None, None),
        P(None, None, "chan", None, None),
        P(None, None, "chan", None, None),
    )
    out_specs = P("edge", None, "chan")
    return jax.shard_map(shards, mesh=mesh, in_specs=in_specs, out_specs=out_specs, check_vma=False)
```
